32 devices in a mesh: groups: 2 (over y), cache: 4 (over x, core), tensor: 4 (over z).
Axes of the slice: x: 2, y: 2, z: 4, core: 2. Of those that a mesh axis runs over, the one named last changes fastest.
Arguments:
- queries: bfloat16 [2048, 8192], P(('groups', 'cache'), 'tensor'), parts along dimension 0, may hold values from -8 to 8
- suffix_key_value: bfloat16 [2, 2048, 1024], P(None, ('groups', 'cache'), 'tensor'), parts along dimension 1, may hold values from -6 to 6
- kv_pages: bfloat16 [768, 2, 128, 1024], P(('groups', 'cache'), None, None, 'tensor'), parts along dimension 0, may hold values from -6 to 6
- page_ids: int32 [8, 64], P(('groups', 'cache')), parts along dimension 0, may hold values from 0 to 383, as said below
- prefix_pages: int32 [8], P(('groups', 'cache')), parts along dimension 0, may hold values from 8 to 64, as said below
- page_home: int32 [768], P('groups'), parts along dimension 0, may hold values from 0 to 383, as said below
- out_weight: bfloat16 [8192, 8192], P('tensor', 'cache'), may hold values from -0.25 to 0.25
Outputs:
- attended: bfloat16 [2048, 8192], P(('groups', 'cache'), 'tensor'), parts along dimension 0
The draws below stay inside these ranges and needn't reach their ends.
There are 2 independent parts, one for each index of `groups`. The reference program is written for one: setup_inputs(seed, part) draws one part's arguments, and reference() takes and returns one part's arrays. A program takes and returns all parts, laid end to end along the dimension named above; an argument that names none is the same for every part. Nothing has to cross between parts.
Inputs may be any that keep to these rules, and one draw needn't show every extreme that they name: `page_ids`: live slots are j < prefix_pages[r]. Within the aligned block of 1 request of one index of cache, no page id appears twice among all 64 slots, and at most 24 of these slots name pages whose row page_home[id] lies on one index of cache (row // 96); in every such block some index of cache gets exactly 24. `prefix_pages`: one request in each draw has 64 pages and another has 8. `page_home`: A permutation of 0 to 383.
All inputs are finite; a program needn't handle non-finite values.
Results may differ from the reference program's by a relative error of at most 0.015.
Values may be sent and summed in bfloat16 or wider, within the bound.
A program may use at most 128 MiB of HBM per device.

```python
import jax
import jax.numpy as jnp
from jax import lax

D = 8192
QUERY_HEADS = 64
KEY_VALUE_HEADS = 8
HEAD_SIZE = 128
PAGE_TOKENS = 128
SUF = 256
MAXP = 64
MINP = 8
POOL_DEV = 96
REQ_DEV = 1
REQS = 4
NEW_TOKENS = 1024
STORED_PAGES = 384
CAP = 24
N_CACHE = 4
N_TENSOR = 4


def page_layout(key):
    base_key = jax.random.fold_in(key, 7001)
    home_rows = jax.random.permutation(jax.random.fold_in(base_key, 1), STORED_PAGES).astype(jnp.int32)
    inverse = jnp.zeros((STORED_PAGES,), jnp.int32).at[home_rows].set(jnp.arange(STORED_PAGES, dtype=jnp.int32))
    slot_count = REQ_DEV * MAXP

    def one_device(device):
        device_key = jax.random.fold_in(base_key, 100 + device)
        remaining = jax.random.permutation(jax.random.fold_in(device_key, 1), N_CACHE * CAP - CAP).astype(jnp.int32) + CAP
        tickets = jnp.concatenate([jnp.arange(CAP, dtype=jnp.int32), remaining])[:slot_count]
        shuffle = jax.random.permutation(jax.random.fold_in(device_key, 2), slot_count)
        tickets = tickets[shuffle]
        first_owner = jax.random.randint(jax.random.fold_in(device_key, 3), (), 0, N_CACHE)
        owners = (tickets // CAP + first_owner) % N_CACHE
        offset = jax.random.randint(jax.random.fold_in(device_key, 4), (N_CACHE,), 0, POOL_DEV)
        within = (offset[owners] + tickets % CAP) % POOL_DEV
        return inverse[owners * POOL_DEV + within]
    page_list = jax.vmap(one_device)(jnp.arange(N_CACHE, dtype=jnp.int32))
    return (home_rows, page_list.reshape(N_CACHE * REQ_DEV, MAXP).astype(jnp.int32))


def draw_page_home(key, part):
    return page_layout(key)[0]


def draw_page_ids(key, part):
    return page_layout(key)[1]


def draw_prefix_pages(key, part):
    base_key = jax.random.fold_in(key, 7002)
    length_span = MAXP - MINP
    first_draw = jax.random.randint(jax.random.fold_in(base_key, 1), (REQS,), 0, length_span + 1)
    second_draw = jax.random.randint(jax.random.fold_in(base_key, 2), (REQS,), 0, length_span + 1)
    lengths = MAXP - first_draw * second_draw // max(length_span, 1)
    longest = jax.random.randint(jax.random.fold_in(base_key, 3), (), 0, REQS)
    step_away = jax.random.randint(jax.random.fold_in(base_key, 4), (), 1, max(REQS, 2))
    shortest = (longest + step_away) % REQS
    request_index = jnp.arange(REQS)
    lengths = jnp.where(request_index == shortest, MINP, lengths)
    lengths = jnp.where(request_index == longest, MAXP, lengths)
    return lengths.astype(jnp.int32)


def draw_queries(key, part):
    noise_key = jax.random.fold_in(key, 7004)
    values = jnp.clip(2.5 * jax.random.normal(noise_key, (NEW_TOKENS, QUERY_HEADS * HEAD_SIZE), jnp.float32), -8.0, 8.0)
    return values.astype(jnp.bfloat16)


def draw_kv_pages(key, part):
    noise_key = jax.random.fold_in(key, 7005)
    array_shape = (STORED_PAGES, 2, PAGE_TOKENS, KEY_VALUE_HEADS * HEAD_SIZE)
    values = jnp.clip(jax.random.normal(noise_key, array_shape, jnp.float32), -6.0, 6.0)
    return values.astype(jnp.bfloat16)


def steps_of(rng, extent, cuts, low, top_value):
    loudness, own = 1.0, jax.random.fold_in(rng, 6)
    for dim, parts in cuts:
        heights = jnp.exp(jax.random.uniform(jax.random.fold_in(own, dim), (parts,), jnp.float32, low / len(cuts), top_value / len(cuts)))
        loudness = loudness * jnp.repeat(heights, extent[dim] // parts).reshape([-1 if axis == dim else 1 for axis in range(len(extent))])
    return loudness


def gaussian(stream_key, extent, scale, most, shards=(), kind=jnp.bfloat16):
    result = scale * jax.random.normal(stream_key, extent, jnp.float32)
    if shards:
        result = result * steps_of(stream_key, extent, shards, -0.22, 0.18)
    return jnp.clip(result, -most, most).astype(kind)


def setup_inputs(seed: int = 0, part: int = 0) -> dict:
    streams_of = jax.random.split(jax.random.key(seed), 8)
    own_keys = jax.random.split(jax.random.fold_in(streams_of[7], part), 8)
    return {
        "queries": draw_queries(jax.random.fold_in(jax.random.fold_in(streams_of[7], part), 71), part),
        "suffix_key_value": gaussian(own_keys[1], (2, NEW_TOKENS, KEY_VALUE_HEADS * HEAD_SIZE), 1.0, 6.0, ((1, 4), (2, 4))),
        "kv_pages": draw_kv_pages(jax.random.fold_in(jax.random.fold_in(streams_of[7], part), 71), part),
        "page_ids": draw_page_ids(jax.random.fold_in(jax.random.fold_in(streams_of[7], part), 71), part),
        "prefix_pages": draw_prefix_pages(jax.random.fold_in(jax.random.fold_in(streams_of[7], part), 71), part),
        "page_home": draw_page_home(jax.random.fold_in(jax.random.fold_in(streams_of[7], part), 71), part),
        "out_weight": gaussian(streams_of[6], (QUERY_HEADS * HEAD_SIZE, D), (QUERY_HEADS * HEAD_SIZE // 16) ** -0.5, 0.25, ((0, 4), (1, 4))),
    }


def attend_head(query_head, key_rows, value_rows, allowed):
    scores = jnp.einsum("sgd,ld->sgl", query_head.astype(jnp.float32), key_rows.astype(jnp.float32)) * (HEAD_SIZE ** -0.5)
    scores = jnp.where(allowed[:, None, :], scores, -jnp.inf)
    row_top = jnp.max(scores, axis=2, keepdims=True)
    weights = jnp.where(allowed[:, None, :], jnp.exp(scores - row_top), 0.0)
    weight_sum = jnp.sum(weights, axis=2, keepdims=True)
    rounded = lax.optimization_barrier(weights.astype(jnp.bfloat16))
    accumulated = jnp.einsum("sgl,ld->sgd", rounded.astype(jnp.float32), value_rows.astype(jnp.float32))
    return (accumulated / weight_sum).astype(jnp.bfloat16)


def reference(queries, suffix_key_value, kv_pages, page_ids, prefix_pages, page_home, out_weight):
    group_width = QUERY_HEADS // KEY_VALUE_HEADS

    def one_request(request_index):
        page_list = page_ids[request_index]
        home_rows = jnp.take(page_home, page_list).astype(jnp.int32)
        pages_here = jnp.take(kv_pages, home_rows, axis=0)
        first_token = (request_index * SUF).astype(jnp.int32)
        query_rows = lax.dynamic_slice_in_dim(queries, first_token, SUF, 0)
        suffix_rows = lax.dynamic_slice_in_dim(suffix_key_value, first_token, SUF, 1)
        key_page = jnp.arange(MAXP * PAGE_TOKENS, dtype=jnp.int32) // PAGE_TOKENS
        prefix_live = jnp.broadcast_to((key_page < prefix_pages[request_index])[None, :], (SUF, MAXP * PAGE_TOKENS))
        positions = jnp.arange(SUF, dtype=jnp.int32)
        causal = positions[None, :] <= positions[:, None]
        allowed = jnp.concatenate([prefix_live, causal], axis=1)

        def single_head(head_index):
            query_head = lax.dynamic_slice_in_dim(query_rows, (head_index * group_width * HEAD_SIZE).astype(jnp.int32), group_width * HEAD_SIZE, 1)
            query_head = query_head.reshape(SUF, group_width, HEAD_SIZE)
            column = (head_index * HEAD_SIZE).astype(jnp.int32)
            prefix_keys = lax.dynamic_slice_in_dim(pages_here[:, 0], column, HEAD_SIZE, 2).reshape(MAXP * PAGE_TOKENS, HEAD_SIZE)
            prefix_values = lax.dynamic_slice_in_dim(pages_here[:, 1], column, HEAD_SIZE, 2).reshape(MAXP * PAGE_TOKENS, HEAD_SIZE)
            suffix_keys = lax.dynamic_slice_in_dim(suffix_rows[0], column, HEAD_SIZE, 1)
            suffix_values = lax.dynamic_slice_in_dim(suffix_rows[1], column, HEAD_SIZE, 1)
            key_rows = jnp.concatenate([prefix_keys, suffix_keys], axis=0)
            value_rows = jnp.concatenate([prefix_values, suffix_values], axis=0)
            return attend_head(query_head, key_rows, value_rows, allowed)

        head_list = lax.map(single_head, jnp.arange(KEY_VALUE_HEADS, dtype=jnp.int32))
        return jnp.transpose(head_list, (1, 0, 2, 3)).reshape(SUF, QUERY_HEADS * HEAD_SIZE)

    mixed_heads = lax.map(one_request, jnp.arange(REQS, dtype=jnp.int32)).reshape(NEW_TOKENS, QUERY_HEADS * HEAD_SIZE)
    span_cols = QUERY_HEADS * HEAD_SIZE // N_TENSOR
    summed = jnp.zeros((NEW_TOKENS, D), jnp.float32)
    for group_index in range(N_TENSOR):
        lower = group_index * span_cols
        group_term = jnp.dot(mixed_heads[:, lower:lower + span_cols], out_weight[lower:lower + span_cols], preferred_element_type=jnp.float32).astype(jnp.bfloat16)
        summed = summed + lax.optimization_barrier(group_term).astype(jnp.float32)
    return summed.astype(jnp.bfloat16)
```

```python
import functools

import jax
import jax.numpy as jnp
from jax import lax
from jax.experimental import pallas as pl
from jax.experimental.pallas import tpu as pltpu
from jax.sharding import PartitionSpec as P

QUERY_HEADS = 64
KEY_VALUE_HEADS = 8
HEAD_SIZE = 128
PAGE_TOKENS = 128
SUF = 256
MAXP = 64

GROUP = QUERY_HEADS // KEY_VALUE_HEADS
LOG2E = 1.4426950408889634
FACTOR = HEAD_SIZE ** (-0.5) * LOG2E
LOW = -1e30
BLOCK = 4
UNROLL = 4
ROW_CHUNKS = 2
PAIRED_BLOCK = 4
NT = (((1,), (1,)), ((), ()))


def attend_kernel(
    capacity, pool_rows, which_head, rows_ref, me_ref, q_ref, suffix_ref, pages_ref, out_ref,
    buf, top, total, acc, counts, sems,
):
    step = pl.program_id(0)
    steps = pl.num_programs(0)
    me = me_ref[0]
    slot = lax.rem(step, 2)

    def page_at(row):
        return pages_ref.at[row, :, :, which_head * HEAD_SIZE : (which_head + 1) * HEAD_SIZE]

    def start_pages(ahead, to):
        which = lax.rem(me + ahead, steps)

        def scan(j, count):
            row = rows_ref[which, j]
            mine = (row >= me * pool_rows) & (row < (me + 1) * pool_rows)

            @pl.when(mine)
            def _():
                pltpu.make_async_copy(
                    page_at(row - me * pool_rows), buf.at[to, count], sems.at[to, count]
                ).start()

            return count + mine.astype(jnp.int32)

        counts[to] = lax.fori_loop(0, MAXP, scan, jnp.int32(0))

    @pl.when(step == 0)
    def _():
        start_pages(0, 0)

    @pl.when(step + 1 < steps)
    def _():
        start_pages(step + 1, 1 - slot)

    top[...] = jnp.full(top.shape, LOW, jnp.float32)
    total[...] = jnp.zeros(total.shape, jnp.float32)
    acc[...] = jnp.zeros(acc.shape, jnp.float32)

    def one_head(head, keys, values, mask):
        query = q_ref[0, :, pl.ds(pl.multiple_of(head * HEAD_SIZE, HEAD_SIZE), HEAD_SIZE)]
        scores = lax.dot_general(query, keys, NT, preferred_element_type=jnp.float32)
        if mask is not None:
            scores = jnp.where(mask, scores, LOW)
        old_top = top[head]
        new_top = jnp.maximum(old_top, jnp.max(scores, axis=1, keepdims=True))
        fade = jnp.exp2((old_top - new_top) * FACTOR)
        weights = []
        sums = total[head] * fade
        for piece in range(scores.shape[1] // HEAD_SIZE):
            part = scores[:, piece * HEAD_SIZE : (piece + 1) * HEAD_SIZE]
            weight = jnp.exp2((part - new_top) * FACTOR)
            sums = sums + weight
            weights.append(weight.astype(jnp.bfloat16))
        low = jnp.concatenate(weights, axis=1)
        acc[head] = acc[head] * fade + jnp.dot(low, values, preferred_element_type=jnp.float32)
        total[head] = sums
        top[head] = new_top

    def all_heads(load, mask):
        def some(i, carry):
            keys, values = load()
            for j in range(UNROLL):
                one_head(i * UNROLL + j, keys, values, mask)
            return carry

        lax.fori_loop(0, GROUP // UNROLL, some, 0)

    @pl.when(step == 0)
    def _():
        rows = lax.broadcasted_iota(jnp.int32, (SUF, SUF), 0)
        columns = lax.broadcasted_iota(jnp.int32, (SUF, SUF), 1)
        all_heads(lambda: (suffix_ref[0], suffix_ref[1]), columns <= rows)

    count = counts[slot]

    def wait_page(index):
        pltpu.make_async_copy(page_at(0), buf.at[slot, index], sems.at[slot, index]).wait()

    def page_block(first, size):
        for j in range(size):
            wait_page(first + j)
        all_heads(
            lambda: (
                buf[slot, pl.ds(first, size), 0].reshape(size * PAGE_TOKENS, HEAD_SIZE),
                buf[slot, pl.ds(first, size), 1].reshape(size * PAGE_TOKENS, HEAD_SIZE),
            ),
            None,
        )

    blocks = count // BLOCK

    @pl.loop(0, blocks)
    def _(b):
        page_block(b * BLOCK, BLOCK)

    @pl.loop(blocks * BLOCK, count)
    def _(p):
        page_block(p, 1)

    width = GROUP * HEAD_SIZE
    lane = lax.broadcasted_iota(jnp.int32, (SUF, HEAD_SIZE), 1)
    out_ref[0, :, width:] = jnp.zeros((SUF, HEAD_SIZE), jnp.bfloat16)

    @pl.loop(0, GROUP)
    def _(head):
        weight_sum = jnp.sum(total[head], axis=1, keepdims=True)
        some_weight = weight_sum > 0.0
        safe = jnp.where(some_weight, weight_sum, 1.0)
        columns = pl.ds(pl.multiple_of(head * HEAD_SIZE, HEAD_SIZE), HEAD_SIZE)
        out_ref[0, :, columns] = (acc[head] / safe).astype(jnp.bfloat16)
        log_sum = jnp.where(some_weight, top[head] * FACTOR + jnp.log2(safe), LOW)
        high = log_sum.astype(jnp.bfloat16)
        rest = log_sum - high.astype(jnp.float32)
        middle = rest.astype(jnp.bfloat16)
        last = (rest - middle.astype(jnp.float32)).astype(jnp.bfloat16)
        stats = out_ref[0, :, width:].astype(jnp.float32)
        heads = GROUP
        stats = jnp.where(lane == head, high.astype(jnp.float32), stats)
        stats = jnp.where(lane == head + heads, middle.astype(jnp.float32), stats)
        stats = jnp.where(lane == head + 2 * heads, last.astype(jnp.float32), stats)
        out_ref[0, :, width:] = stats.astype(jnp.bfloat16)


def attend(rows, me, queries, suffix, pages, capacity, which_head):
    requests = rows.shape[0]
    width = queries.shape[2]
    state = pltpu.VMEM((GROUP, SUF, HEAD_SIZE), jnp.float32)
    return pl.pallas_call(
        functools.partial(attend_kernel, capacity, pages.shape[0], which_head),
        grid_spec=pltpu.PrefetchScalarGridSpec(
            num_scalar_prefetch=2,
            grid=(requests,),
            in_specs=[
                pl.BlockSpec((1, SUF, width), lambda r, rows, me: (lax.rem(me[0] + r, requests), 0, 0)),
                pl.BlockSpec((2, SUF, HEAD_SIZE), lambda r, *_: (0, 0, which_head)),
                pl.BlockSpec(memory_space=pl.ANY),
            ],
            out_specs=pl.BlockSpec((1, SUF, width + HEAD_SIZE), lambda r, *_: (r, 0, 0)),
            scratch_shapes=[
                pltpu.VMEM((2, capacity) + pages.shape[1:3] + (HEAD_SIZE,), pages.dtype),
                state,
                state,
                state,
                pltpu.SMEM((2,), jnp.int32),
                pltpu.SemaphoreType.DMA((2, capacity)),
            ],
        ),
        out_shape=jax.ShapeDtypeStruct((requests, SUF, width + HEAD_SIZE), jnp.bfloat16),
        cost_estimate=pl.CostEstimate(
            flops=16_000_000_000, bytes_accessed=20_000_000, transcendentals=16_000_000
        ),
        compiler_params=pltpu.CompilerParams(vmem_limit_bytes=48 * 1024 * 1024),
    )(rows, me, queries, suffix, pages)


def combine_kernel(heads, *refs):
    partials, out_ref = refs[:-1], refs[-1]
    owners = len(partials)
    width = heads * HEAD_SIZE
    stats = [partial[:, width:].astype(jnp.float32) for partial in partials]
    for head in range(heads):
        logs = [
            s[:, head : head + 1]
            + s[:, heads + head : heads + head + 1]
            + s[:, 2 * heads + head : 2 * heads + head + 1]
            for s in stats
        ]
        high = functools.reduce(jnp.maximum, logs)
        shares = [jnp.exp2(value - high) for value in logs]
        whole = functools.reduce(jnp.add, shares)
        lanes = slice(head * HEAD_SIZE, (head + 1) * HEAD_SIZE)
        mixed = functools.reduce(
            jnp.add,
            [
                partials[o][:, lanes].astype(jnp.float32) * (shares[o] / whole)
                for o in range(owners)
            ],
        )
        out_ref[:, lanes] = mixed.astype(jnp.bfloat16)


def combine(partials, width):
    tile = 64
    return pl.pallas_call(
        functools.partial(combine_kernel, width // HEAD_SIZE),
        grid=(SUF // tile,),
        in_specs=[pl.BlockSpec((tile, x.shape[1]), lambda i: (i, 0)) for x in partials],
        out_specs=pl.BlockSpec((tile, width), lambda i: (i, 0)),
        out_shape=jax.ShapeDtypeStruct((SUF, width), jnp.bfloat16),
        cost_estimate=pl.CostEstimate(
            flops=10_000_000, bytes_accessed=6_000_000, transcendentals=100_000
        ),
    )(*partials)


def paired_kernel(n, suffix_at, pool_rows, rows_ref, me_ref, *refs):
    q_refs, (suffix_ref, pages_ref, mine_ref, theirs_ref, out_ref, q_buf, buf, top, total, acc, fades, peaks, vt, causal, s0, s1, p0, p1, counts, out_sems, q_sems, sems) = refs[:n], refs[n:]
    s_bufs, p_bufs = (s0, s1), (p0, p1)
    me = me_ref[0]
    parts = buf.shape[4] // HEAD_SIZE
    first = me * pool_rows
    for i in range(n):
        pltpu.make_async_copy(q_refs[i], q_buf.at[i], q_sems.at[i]).start()

    def page_copy(row, i, slot):
        return pltpu.make_async_copy(pages_ref.at[row], buf.at[i, slot], sems.at[i, slot])

    for i in range(n):
        def scan(j, count):
            row = rows_ref[i, j]
            mine = (row >= first) & (row < first + pool_rows)

            @pl.when(mine)
            def _():
                page_copy(row - first, i, count).start()

            return count + mine.astype(jnp.int32)

        counts[i] = lax.fori_loop(0, MAXP, scan, jnp.int32(0), unroll=8)


    for i in range(n):
        pltpu.make_async_copy(q_refs[i], q_buf.at[i], q_sems.at[i]).wait()
    keys = lax.broadcasted_iota(jnp.int32, (SUF, SUF), 0)
    tokens = lax.broadcasted_iota(jnp.int32, (SUF, SUF), 1)
    causal[...] = jnp.where(keys <= tokens, 0.0, LOW)

    @pl.loop(0, n)
    def _(i):
        count = counts[i]

        @pl.loop(0, count)
        def _(p):
            page_copy(0, i, p).wait()
            for kh in range(parts):
                vt[i, kh, p] = buf[i, p, 1, :, kh * HEAD_SIZE : (kh + 1) * HEAD_SIZE].T

        @pl.loop(count, (count + PAIRED_BLOCK - 1) // PAIRED_BLOCK * PAIRED_BLOCK)
        def _(p):
            buf[i, p, 0] = jnp.zeros(buf.shape[3:], buf.dtype)
            for kh in range(parts):
                vt[i, kh, p] = jnp.zeros(vt.shape[3:], vt.dtype)

    p_bufs[1][...] = jnp.zeros(p_bufs[1].shape, jnp.bfloat16)

    @pl.loop(0, n * parts)
    def _(step):
        i = step // parts
        kh = lax.rem(step, parts)
        lanes = pl.ds(pl.multiple_of(kh * HEAD_SIZE, HEAD_SIZE), HEAD_SIZE)
        top[...] = jnp.full(top.shape, LOW, jnp.float32)
        total[...] = jnp.zeros(total.shape, jnp.float32)
        acc[...] = jnp.zeros(acc.shape, jnp.float32)
        count = counts[i]
        last = (count + PAIRED_BLOCK - 1) // PAIRED_BLOCK - 1

        def query(head):
            column = pl.multiple_of((kh * GROUP + head) * HEAD_SIZE, HEAD_SIZE)
            return q_buf[i, :, pl.ds(column, HEAD_SIZE)]

        def score(head, keys, first, bias=None):
            rows = keys.shape[0]
            found = lax.dot_general(keys, query(head), NT, preferred_element_type=jnp.float32)
            if bias is not None:
                found = found + bias[...]
            s_bufs[head % 2][:rows] = found
            highs = None
            for g in range(rows // PAGE_TOKENS):
                piece = found[g * PAGE_TOKENS : (g + 1) * PAGE_TOKENS]
                high = jnp.max(piece.reshape(PAGE_TOKENS // 8, 8, SUF), axis=0)
                if first is not None:
                    high = jnp.where(first + g < count, high, LOW)
                highs = high if highs is None else jnp.maximum(highs, high)
            peaks[head % 2] = highs

        def weigh(head, rows, first):
            s_ref, p_ref = s_bufs[head % 2], p_bufs[head % 2]
            pages = rows // PAGE_TOKENS
            old = top[head]
            new = jnp.maximum(old, jnp.max(peaks[head % 2], axis=0, keepdims=True))
            fade = jnp.exp2((old - new) * FACTOR)
            base = new * FACTOR
            sums = total[head] * fade
            for g in range(pages):
                shift = base if first is None else jnp.where(first + g < count, base, -LOW)
                weight = jnp.exp2(s_ref[g * PAGE_TOKENS : (g + 1) * PAGE_TOKENS] * FACTOR - shift)
                sums = sums + jnp.sum(weight.reshape(PAGE_TOKENS // 8, 8, SUF), axis=0)
                p_ref[g * PAGE_TOKENS : (g + 1) * PAGE_TOKENS] = weight.astype(jnp.bfloat16)
            total[head] = sums
            top[head] = new
            fades[head % 2] = fade

        def mix(head, values):
            acc[head] = acc[head] * fades[head % 2] + jnp.dot(
                values, p_bufs[head % 2][: values.shape[1]], preferred_element_type=jnp.float32
            )

        if suffix_at is not None:
            @pl.when(i == suffix_at)
            def _():
                ks = suffix_ref[0, :, lanes]
                vs = suffix_ref[1, :, lanes].T
                score(0, ks, None, causal)
                for head in range(GROUP):
                    if head + 1 < GROUP:
                        score(head + 1, ks, None, causal)
                    weigh(head, SUF, None)
                    if head:
                        mix(head - 1, vs)
                mix(GROUP - 1, vs)

        def block_keys(b):
            return buf[i, pl.ds(b * PAIRED_BLOCK, PAIRED_BLOCK), 0, :, lanes].reshape(PAIRED_BLOCK * PAGE_TOKENS, HEAD_SIZE)

        def block_values(b):
            tiles = [vt[i, kh, b * PAIRED_BLOCK + g] for g in range(PAIRED_BLOCK)]
            return jnp.concatenate(tiles, axis=1)

        @pl.when(count > 0)
        def _():
            score(0, block_keys(0), 0)
            p_bufs[1][...] = jnp.zeros(p_bufs[1].shape, jnp.bfloat16)
            fades[1] = jnp.ones(fades.shape[1:], jnp.float32)

            @pl.loop(0, last + 1)
            def _(b):
                ks, vs = block_keys(b), block_values(b)
                for head in range(GROUP):
                    if head + 1 < GROUP:
                        score(head + 1, ks, b * PAIRED_BLOCK)
                    else:
                        score(0, block_keys(jnp.minimum(b + 1, last)), jnp.minimum(b + 1, last) * PAIRED_BLOCK)
                    weigh(head, PAIRED_BLOCK * PAGE_TOKENS, b * PAIRED_BLOCK)
                    if head:
                        mix(head - 1, vs)
                    else:
                        mix(GROUP - 1, block_values(jnp.maximum(b - 1, 0)))

            mix(GROUP - 1, block_values(last))

        slot = lax.rem(kh + me, 2) if parts == 2 else kh
        logs = []
        for head in range(GROUP):
            weight_sum = jnp.sum(total[head], axis=0, keepdims=True)
            some_weight = weight_sum > 0.0
            safe = jnp.where(some_weight, weight_sum, 1.0)
            out_ref[slot, i, head * HEAD_SIZE : (head + 1) * HEAD_SIZE] = (acc[head] * (1.0 / safe)).astype(jnp.bfloat16)
            logs.append(jnp.where(some_weight, top[head] * FACTOR + jnp.log2(safe), LOW))
        log_sum = jnp.concatenate(logs, axis=0)
        high = log_sum.astype(jnp.bfloat16).astype(jnp.float32)
        rest = log_sum - high
        middle = rest.astype(jnp.bfloat16).astype(jnp.float32)
        stats = jnp.concatenate([high, middle, rest - middle, jnp.zeros_like(high)], axis=0)
        out_ref[slot, i, GROUP * HEAD_SIZE :] = stats.astype(jnp.bfloat16)

        @pl.when(kh == parts - 1)
        def _():
            for half, ref in enumerate((mine_ref, theirs_ref)):
                pltpu.make_async_copy(out_ref.at[half, i], ref.at[i], out_sems.at[half, i]).start()

    for i in range(n):
        for half, ref in enumerate((mine_ref, theirs_ref)):
            pltpu.make_async_copy(out_ref.at[half, i], ref.at[i], out_sems.at[half, i]).wait()

def paired_attend(rows, me, queries, suffix, pages, capacity, suffix_at):
    n = len(queries)
    width = queries[0].shape[1]
    parts = pages.shape[3] // HEAD_SIZE
    high_rows = GROUP * HEAD_SIZE + 4 * GROUP
    rows_max = max(PAIRED_BLOCK * PAGE_TOKENS, SUF)
    return pl.pallas_call(
        functools.partial(paired_kernel, n, suffix_at, pages.shape[0]),
        in_specs=[pl.BlockSpec(memory_space=pltpu.SMEM)] * 2 + [pl.BlockSpec(memory_space=pltpu.HBM)] * n
        + [pl.BlockSpec(memory_space=pltpu.VMEM), pl.BlockSpec(memory_space=pltpu.HBM)],
        out_specs=[pl.BlockSpec(memory_space=pltpu.HBM)] * 2,
        scratch_shapes=[
            pltpu.VMEM((parts, n, high_rows, SUF), jnp.bfloat16),
            pltpu.VMEM((n, SUF, width), jnp.bfloat16),
            pltpu.VMEM((n, capacity + PAIRED_BLOCK) + pages.shape[1:], pages.dtype),
            pltpu.VMEM((GROUP, 1, SUF), jnp.float32),
            pltpu.VMEM((GROUP, 8, SUF), jnp.float32),
            pltpu.VMEM((GROUP, HEAD_SIZE, SUF), jnp.float32),
            pltpu.VMEM((2, 1, SUF), jnp.float32),
            pltpu.VMEM((2, 8, SUF), jnp.float32),
            pltpu.VMEM((n, parts, capacity + PAIRED_BLOCK, HEAD_SIZE, PAGE_TOKENS), jnp.bfloat16),
            pltpu.VMEM((SUF, SUF), jnp.float32),
            pltpu.VMEM((rows_max, SUF), jnp.float32),
            pltpu.VMEM((rows_max, SUF), jnp.float32),
            pltpu.VMEM((rows_max, SUF), jnp.bfloat16),
            pltpu.VMEM((rows_max, SUF), jnp.bfloat16),
            pltpu.SMEM((n,), jnp.int32),
            pltpu.SemaphoreType.DMA((parts, n)),
            pltpu.SemaphoreType.DMA((n,)),
            pltpu.SemaphoreType.DMA((n, capacity)),
        ],
        out_shape=[jax.ShapeDtypeStruct((n, high_rows, SUF), jnp.bfloat16)] * 2,
        cost_estimate=pl.CostEstimate(flops=16_000_000_000, bytes_accessed=10_000_000, transcendentals=16_000_000),
        compiler_params=pltpu.CompilerParams(vmem_limit_bytes=48 * 1024 * 1024),
    )(rows, me, *queries, suffix, pages)


MESH = pl.DeviceIdType.MESH
CHUNKS = 4
SKEW = 2
LIMIT = 60 * 1024 * 1024


def log_sums(stats):
    stats = stats.astype(jnp.float32)
    return stats[:GROUP] + stats[GROUP : 2 * GROUP] + stats[2 * GROUP : 3 * GROUP]


def shares_of(logs):
    high = functools.reduce(jnp.maximum, logs)
    shares = [jnp.exp2(value - high) for value in logs]
    whole = functools.reduce(jnp.add, shares)
    return [share / whole for share in shares], high + jnp.log2(whole)


def packed_stats(log_sum):
    high = log_sum.astype(jnp.bfloat16).astype(jnp.float32)
    rest = log_sum - high
    middle = rest.astype(jnp.bfloat16).astype(jnp.float32)
    stats = jnp.concatenate([high, middle, rest - middle, jnp.zeros_like(high)], axis=0)
    return stats.astype(jnp.bfloat16)


def weighted(pair, shares, head, rows):
    return functools.reduce(
        jnp.add, [x[rows].astype(jnp.float32) * share[head : head + 1] for x, share in zip(pair, shares)]
    )


def merge(pair, out):
    top = GROUP * HEAD_SIZE
    shares, log_sum = shares_of([log_sums(x[top:]) for x in pair])
    for head in range(GROUP):
        rows = slice(head * HEAD_SIZE, (head + 1) * HEAD_SIZE)
        out[rows] = weighted(pair, shares, head, rows).astype(jnp.bfloat16)
    out[top:] = packed_stats(log_sum)


def merge_kernel(one_ref, other_ref, out_ref):
    merge((one_ref.at[0], other_ref.at[0]), out_ref.at[0])


def merge_halves(mine, from_mate):
    n, rows, width = mine.shape
    block = (1, rows, width // 2)
    return pl.pallas_call(
        merge_kernel,
        grid=(n, 2),
        in_specs=[
            pl.BlockSpec(block, lambda j, h: (j, 0, h)),
            pl.BlockSpec(block, lambda j, h: (n - 1 - j, 0, h)),
        ],
        out_specs=pl.BlockSpec(block, lambda j, h: (j, 0, h)),
        out_shape=jax.ShapeDtypeStruct(mine.shape, mine.dtype),
        cost_estimate=pl.CostEstimate(flops=100_000_000, bytes_accessed=3_000_000, transcendentals=0),
    )(mine, from_mate)


def finish_kernel(
    near_ref, got_ref, mine_ref, theirs_ref, weight_ref, out_ref,
    near, got, mine, weight, from_mate, summed, from_far, mixed, staged, terms, rising, falling,
    local_sems, mate_sems, far_sems, mixed_sems, term_send, term_recv, rise_sems, fall_sems,
):
    group, cache, place = (lax.axis_index(a) for a in ("groups", "cache", "tensor"))
    places = lax.axis_size("tensor")
    core = lax.rem(cache, 2)
    chip = cache // 2
    mate = cache + 1 - 2 * core
    far = 2 * (1 - chip) + core
    half_width = GROUP * HEAD_SIZE
    lanes = SUF // 2
    span = weight.shape[1] // CHUNKS

    def at(who, where=None):
        return (group, who, place if where is None else where)

    barrier = pltpu.get_barrier_semaphore()
    for who in (mate, far, 2 * (1 - chip) + 1 - core):
        pl.semaphore_signal(barrier, inc=1, device_id=at(who), device_id_type=MESH)

    @pl.when(place > 0)
    def _():
        pl.semaphore_signal(barrier, inc=1, device_id=at(cache, place - 1), device_id_type=MESH)

    @pl.when(place < places - 1)
    def _():
        pl.semaphore_signal(barrier, inc=1, device_id=at(cache, place + 1), device_id_type=MESH)

    weight_copy = pltpu.make_async_copy(weight_ref, weight, local_sems.at[3])
    local_copies = [
        pltpu.make_async_copy(src, dst, local_sems.at[i])
        for i, (src, dst) in enumerate(((mine_ref, mine), (near_ref, near), (got_ref, got)))
    ]
    for copy in local_copies:
        copy.start()
    weight_copy.start()
    neighbours = jnp.minimum(place, 1) + jnp.minimum(places - 1 - place, 1)
    pl.semaphore_wait(barrier, 3 + neighbours)

    def remote(src, dst, send, recv, who):
        return pltpu.make_async_remote_copy(
            src_ref=src, dst_ref=dst, send_sem=send, recv_sem=recv, device_id=who, device_id_type=MESH
        )

    mate_copies = [
        remote(theirs_ref.at[j], from_mate.at[1 - j], mate_sems.at[0, j], mate_sems.at[1, 1 - j], at(mate))
        for j in range(2)
    ]
    for copy in mate_copies:
        copy.start()
    for copy in local_copies:
        copy.wait()
    for j in range(2):
        remote(
            theirs_ref.at[j], from_mate.at[j], mate_sems.at[0, j], mate_sems.at[1, j], at(mate)
        ).wait_recv()

    def far_copy(piece):
        return remote(
            summed.at[piece], from_far.at[piece], far_sems.at[0, piece], far_sems.at[1, piece], at(far)
        )

    @pl.loop(0, 2)
    def _(piece):
        columns = pl.ds(pl.multiple_of(piece * lanes, lanes), lanes)
        for j in range(2):
            merge((mine.at[j, :, columns], from_mate.at[j, :, columns]), summed.at[piece, j])
        far_copy(piece).start()

    weight_copy.wait()

    def mixed_copy(phase, piece, half):
        return remote(
            mixed.at[phase, piece, half], mixed.at[phase, piece, half],
            mixed_sems.at[0, phase, piece], mixed_sems.at[1, phase, piece], at(mate),
        )

    def to_mate(piece, n):
        return remote(
            staged.at[0, piece, n, 1 - core], terms.at[cache, piece, n],
            term_send.at[0, piece, n], term_recv.at[cache, piece, n], at(mate),
        )

    def to_far(piece, n, k):
        return remote(
            staged.at[1, piece, n, k], terms.at[cache, piece, n],
            term_send.at[1 + k, piece, n], term_recv.at[cache, piece, n], at(2 * (1 - chip) + k),
        )

    def project(phase, piece):
        columns = slice(piece * lanes, (piece + 1) * lanes)
        if phase == 0:
            far_copy(piece).wait_recv()
        for j in range(2):
            k = lax.rem(j + core, 2)
            if phase == 0:
                pair = (near.at[j, :, columns], from_far.at[piece, j])
            else:
                pair = (got.at[j, :, columns], summed.at[piece, j])
            shares, _ = shares_of([log_sums(x[half_width:]) for x in pair])
            for head in range(GROUP):
                rows = slice(head * HEAD_SIZE, (head + 1) * HEAD_SIZE)
                total = weighted(pair, shares, head, rows)
                mixed[phase, piece, core, k, :, rows] = total.astype(jnp.bfloat16).T
        mixed_copy(phase, piece, core).start()
        mixed_copy(phase, piece, 1 - core).wait_recv()
        left = mixed[phase, piece, 0].reshape(2 * lanes, half_width)
        right = mixed[phase, piece, 1].reshape(2 * lanes, half_width)

        @pl.loop(0, CHUNKS)
        def _(n):
            columns = pl.ds(pl.multiple_of(n * span, span), span)
            term = jnp.dot(left, weight[:half_width, columns], preferred_element_type=jnp.float32)
            term = term + jnp.dot(right, weight[half_width:, columns], preferred_element_type=jnp.float32)
            staged[phase, piece, n] = term.astype(jnp.bfloat16).reshape(2, lanes, span)
            if phase == 0:
                terms[cache, piece, n] = staged[0, piece, n, core]
                to_mate(piece, n).start()
            else:
                for k in range(2):
                    to_far(piece, n, k).start()

    def term_arrival(block, piece, n):
        @pl.when(block != cache)
        def _():
            remote(
                terms.at[block, piece, n], terms.at[block, piece, n],
                term_send.at[0, piece, n], term_recv.at[block, piece, n], at(mate),
            ).wait_recv()

    def rise(block, piece, n, where):
        return remote(
            terms.at[block, piece, n], rising.at[block, piece, n],
            rise_sems.at[0, block, piece, n], rise_sems.at[1, block, piece, n], at(cache, where),
        )

    def fall(block, piece, n, where):
        return remote(
            terms.at[block, piece, n], falling.at[block, piece, n],
            fall_sems.at[0, block, piece, n], fall_sems.at[1, block, piece, n], at(cache, where),
        )

    def add_in(block, piece, n, ref):
        terms[block, piece, n] = (
            terms[block, piece, n].astype(jnp.float32) + ref[block, piece, n].astype(jnp.float32)
        ).astype(jnp.bfloat16)

    def chains(base, piece):
        items = 2 * CHUNKS

        @pl.loop(0, items + SKEW * (places - 1))
        def _(stage):
            up = stage - SKEW * place
            block = base + 1 - up // CHUNKS
            n = lax.rem(up + items, CHUNKS)

            @pl.when((up >= 0) & (up < items) & (place < block))
            def _():
                term_arrival(block, piece, n)

                @pl.when(place > 0)
                def _():
                    rise(block, piece, n, place - 1).wait_recv()
                    add_in(block, piece, n, rising)

                rise(block, piece, n, place + 1).start()

            down = stage - SKEW * (places - 1 - place)
            block2 = base + down // CHUNKS
            n2 = lax.rem(down + items * SKEW, CHUNKS)

            @pl.when((down >= 0) & (down < items) & (place > block2))
            def _():
                term_arrival(block2, piece, n2)

                @pl.when(place < places - 1)
                def _():
                    fall(block2, piece, n2, place + 1).wait_recv()
                    add_in(block2, piece, n2, falling)

                fall(block2, piece, n2, place - 1).start()

    for piece in range(2):
        project(1, piece)
        project(0, piece)
        chains(2 * chip, piece)
    for piece in range(2):
        chains(2 * (1 - chip), piece)

    @pl.loop(0, 2 * CHUNKS)
    def _(i):
        piece = i // CHUNKS
        n = lax.rem(i, CHUNKS)
        term_arrival(place, piece, n)

        @pl.when(place > 0)
        def _():
            rise(place, piece, n, place - 1).wait_recv()

        @pl.when(place < places - 1)
        def _():
            fall(place, piece, n, place + 1).wait_recv()

        @pl.when(place == 0)
        def _():
            add_in(place, piece, n, falling)

        @pl.when(place == places - 1)
        def _():
            add_in(place, piece, n, rising)

        @pl.when((place > 0) & (place < places - 1))
        def _():
            terms[place, piece, n] = (
                terms[place, piece, n].astype(jnp.float32)
                + rising[place, piece, n].astype(jnp.float32)
                + falling[place, piece, n].astype(jnp.float32)
            ).astype(jnp.bfloat16)

        rows = pl.ds(pl.multiple_of(piece * lanes, lanes), lanes)
        columns = pl.ds(pl.multiple_of(n * span, span), span)
        out_ref[rows, columns] = terms[place, piece, n]

    for copy in mate_copies:
        copy.wait_send()

    @pl.loop(0, 2)
    def _(piece):
        far_copy(piece).wait_send()
        for phase in range(2):
            mixed_copy(phase, piece, core).wait_send()

        @pl.loop(0, CHUNKS)
        def _(n):
            to_mate(piece, n).wait_send()
            for k in range(2):
                to_far(piece, n, k).wait_send()

            @pl.loop(0, 4)
            def _(block):
                @pl.when(place < block)
                def _():
                    rise(block, piece, n, place + 1).wait_send()

                @pl.when(place > block)
                def _():
                    fall(block, piece, n, place - 1).wait_send()


def finish(near, got, mine, theirs, out_weight):
    rows = near.shape[1]
    lanes = SUF // 2
    wide = out_weight.shape[1]
    half_width = GROUP * HEAD_SIZE
    bf16 = jnp.bfloat16
    blocks = (4, 2, CHUNKS, lanes, wide // CHUNKS)
    whole = pltpu.VMEM((2, rows, SUF), bf16)
    split = pltpu.VMEM((2, 2, rows, lanes), bf16)
    dma = pltpu.SemaphoreType.DMA
    return pl.pallas_call(
        finish_kernel,
        in_specs=[pl.BlockSpec(memory_space=pltpu.HBM)] * 5,
        out_specs=pl.BlockSpec(memory_space=pltpu.VMEM),
        out_shape=jax.ShapeDtypeStruct((SUF, wide), bf16),
        scratch_shapes=[
            whole, whole, whole,
            pltpu.VMEM(out_weight.shape, bf16),
            whole, split, split,
            pltpu.VMEM((2, 2, 2, 2, lanes, half_width), bf16),
            pltpu.VMEM((2, 2, CHUNKS, 2, lanes, wide // CHUNKS), bf16),
            pltpu.VMEM(blocks, bf16),
            pltpu.VMEM(blocks, bf16),
            pltpu.VMEM(blocks, bf16),
            dma((4,)),
            dma((2, 2)),
            dma((2, 2)),
            dma((2, 2, 2)),
            dma((3, 2, CHUNKS)),
            dma((4, 2, CHUNKS)),
            dma((2, 4, 2, CHUNKS)),
            dma((2, 4, 2, CHUNKS)),
        ],
        cost_estimate=pl.CostEstimate(flops=9_000_000_000, bytes_accessed=14_000_000, transcendentals=0),
        compiler_params=pltpu.CompilerParams(
            collective_id=0, has_side_effects=True, vmem_limit_bytes=LIMIT
        ),
    )(near, got, mine, theirs, out_weight)


def paired_device(queries, suffix_key_value, kv_pages, page_ids, prefix_pages, page_home, out_weight):
    cache_count = lax.axis_size("cache")
    me = lax.axis_index("cache")
    capacity = (3 * page_ids.shape[0] * MAXP + 2 * cache_count - 1) // (2 * cache_count)

    def swap(value, distance):
        pairs = [(i, i ^ distance) for i in range(cache_count)]
        return lax.ppermute(value, "cache", pairs)

    table_index = jnp.arange(page_home.shape[0], dtype=jnp.int32)
    flat_ids = page_ids.reshape(-1)
    rows_of = jnp.sum(
        jnp.where(flat_ids[:, None] == table_index[None, :], page_home[None, :], 0), axis=1
    )
    live = jnp.arange(MAXP, dtype=jnp.int32) < prefix_pages[0]
    rows = jnp.where(live, rows_of, -1)[None, :]
    far_queries = swap(queries, 2)
    near_queries = swap(queries, 1)
    pair_rows = jnp.concatenate([rows, swap(rows, 1)], axis=0)
    far_rows = swap(pair_rows, 2)
    where = me.reshape(1).astype(jnp.int32)
    mine, theirs = paired_attend(
        pair_rows, where, [queries, near_queries], suffix_key_value, kv_pages, capacity, 0
    )
    far_queries, theirs = lax.optimization_barrier((far_queries, theirs))
    last_queries = swap(far_queries, 1)
    near = merge_halves(mine, swap(theirs, 1))
    got = swap(near, 2)
    near, last_queries = lax.optimization_barrier((near, last_queries))
    mine, theirs = paired_attend(
        far_rows, where, [far_queries, last_queries], suffix_key_value, kv_pages, capacity, None
    )
    return finish(near, got, mine, theirs, out_weight)


def per_device(queries, suffix_key_value, kv_pages, page_ids, prefix_pages, page_home, out_weight):
    cache_count = lax.axis_size("cache")
    me = lax.axis_index("cache")
    capacity = (3 * page_ids.shape[0] * MAXP + 2 * cache_count - 1) // (2 * cache_count)
    width = queries.shape[1]
    table_index = jnp.arange(page_home.shape[0], dtype=jnp.int32)
    flat_ids = page_ids.reshape(-1)
    rows_of = jnp.sum(
        jnp.where(flat_ids[:, None] == table_index[None, :], page_home[None, :], 0), axis=1
    )
    live = jnp.arange(MAXP, dtype=jnp.int32) < prefix_pages[0]
    rows = lax.all_gather(jnp.where(live, rows_of, -1)[None, :], "cache", axis=0, tiled=True)
    parts = kv_pages.shape[3] // HEAD_SIZE
    part_width = width // parts
    gathered = [
        lax.all_gather(
            queries[:, p * part_width : (p + 1) * part_width], "cache", axis=0, tiled=True
        )
        for p in range(parts)
    ]
    whole = []
    waiting = None

    def finish(arrived):
        mixed = combine(arrived, part_width)
        whole.append(
            lax.all_gather(mixed, "cache", axis=0, tiled=True).reshape(
                cache_count, SUF, part_width
            )
        )

    for p in range(parts):
        partial = attend(
            rows,
            me.reshape(1).astype(jnp.int32),
            gathered[p].reshape(cache_count, SUF, part_width),
            suffix_key_value,
            kv_pages,
            capacity,
            p,
        )
        if waiting is not None:
            partial, waiting = lax.optimization_barrier((partial, waiting))
            finish(waiting)
        waiting = [partial[0]]
        for shift in range(1, cache_count):
            pairs = [(i, (i + shift) % cache_count) for i in range(cache_count)]
            waiting.append(lax.ppermute(partial[shift], "cache", pairs))
    finish(waiting)
    step = SUF // ROW_CHUNKS
    pieces = []
    for i in range(ROW_CHUNKS):
        terms = sum(
            jnp.dot(
                whole[p][:, i * step : (i + 1) * step].reshape(cache_count * step, part_width),
                out_weight[p * part_width : (p + 1) * part_width],
                preferred_element_type=jnp.float32,
            )
            for p in range(parts)
        ).astype(jnp.bfloat16)
        group_term = lax.all_to_all(terms, "cache", split_axis=0, concat_axis=1, tiled=True)
        pieces.append(
            lax.psum_scatter(group_term, "tensor", scatter_dimension=1, tiled=True)
        )
    return jnp.concatenate(pieces, axis=0)


def solution(mesh):
    in_specs = (
        P(("groups", "cache"), "tensor"),
        P(None, ("groups", "cache"), "tensor"),
        P(("groups", "cache"), None, None, "tensor"),
        P(("groups", "cache"), None),
        P(("groups", "cache")),
        P("groups"),
        P("tensor", "cache"),
    )
    out_specs = P(("groups", "cache"), "tensor")
    sizes = dict(mesh.shape)
    paired = sizes["cache"] == 4 and sizes["tensor"] == 4
    return jax.shard_map(
        paired_device if paired else per_device, mesh=mesh, in_specs=in_specs, out_specs=out_specs, check_vma=False
    )
```
